256 devices in a mesh: dp: 8 (over x, y_lo), expert: 16 (over z, core), tensor: 2 (over y_hi).
Axes of the slice: x: 4, y: 4 (y_hi: 2, y_lo: 2; y = y_hi * 2 + y_lo), z: 8, core: 2. Of those that a mesh axis runs over, the one named last changes fastest.
Arguments:
- tokens: bfloat16 [1536, 256, 1280], P(('dp', 'expert', 'tensor')), may hold values from -16 to 16
- cotangent: bfloat16 [1536, 256, 1280], P(('dp', 'expert', 'tensor')), may hold values from -6 to 6
- norm_gain: float32 [1280], replicated, may hold values from 0.5 to 1.5
- slot_keys: bfloat16 [1280, 32], replicated, may hold values from -2 to 2
- w_in: bfloat16 [16, 1280, 2560], P('expert', None, 'tensor'), may hold values from -0.15625 to 0.15625
- w_out: bfloat16 [16, 2560, 1280], P('expert', 'tensor'), may hold values from -0.125 to 0.125
Outputs:
- grad_tokens: bfloat16 [1536, 256, 1280], P(('dp', 'expert', 'tensor'))
- grad_gain: float32 [1280], replicated
- grad_keys: float32 [1280, 32], replicated
- grad_in: bfloat16 [16, 1280, 2560], P('expert', 'dp', 'tensor')
- grad_out: bfloat16 [16, 2560, 1280], P('expert', 'tensor', 'dp')
The draws below stay inside these ranges and needn't reach their ends.
All inputs are finite; a program needn't handle non-finite values.
Results may differ from the reference program's by a relative error of at most 0.014.
The reference program's roundings to bfloat16 on the way count: a program that leaves them out, or rounds other values in their place, can miss the bound.
Values may be sent and summed in bfloat16 or wider, within the bound.
A program may use at most 128 MiB of HBM per device.

```python
import math
import jax
import jax.numpy as jnp
from jax import lax

D = 1280
TOK_IMG = 256
SLOT_PER = 2
FF = 2560
IMG_DEV = 6
EXPERTS = 16
SLOTS = 32
IMAGES = 1536


def draw_slot_keys(key, part):
    values = jax.random.normal(jax.random.fold_in(key, 11), (D, SLOTS), jnp.float32) * (1.0 / math.sqrt(D))
    limit = 1.0 + 2000 // D
    return jnp.clip(values, -limit, limit).astype(jnp.bfloat16)


def draw_tokens(key, part):
    values = jax.random.normal(jax.random.fold_in(key, 21), (IMAGES, TOK_IMG, D), jnp.float32)
    return jnp.clip(values, -16.0, 16.0).astype(jnp.bfloat16)


def level_of(rng, shape, split, smallest, largest):
    factor_of = 1.0
    for dim, blocks in split:
        draws = jax.random.uniform(jax.random.fold_in(jax.random.fold_in(rng, 6), dim), (blocks,), jnp.float32, smallest / len(split), largest / len(split))
        factor_of = factor_of * jnp.repeat(jnp.exp(draws), shape[dim] // blocks).reshape((-1,) + (1,) * (len(shape) - 1 - dim))
    return factor_of


def bell_draw(rng, extent, scale, most, split=(), dtype=jnp.bfloat16):
    values = scale * jax.random.normal(rng, extent, jnp.float32)
    if split:
        values = values * level_of(rng, extent, split, -0.22, 0.18)
    return jnp.clip(values, -most, most).astype(dtype)


def setup_inputs(seed: int = 0) -> dict:
    arg_keys = jax.random.split(jax.random.key(seed), 7)
    tokens = draw_tokens(jax.random.fold_in(arg_keys[6], 71), 0)
    cotangent = bell_draw(arg_keys[1], (IMAGES, TOK_IMG, D), 1.0, 6.0, ((0, 256),))
    norm_gain = jnp.clip(1.0 + 0.1 * jax.random.normal(arg_keys[2], (D,), jnp.float32), 0.5, 1.5)
    slot_keys = draw_slot_keys(jax.random.fold_in(arg_keys[6], 71), 0)
    w_in = bell_draw(arg_keys[4], (EXPERTS, D, FF), D ** -0.5, 0.15625, ((0, 16), (2, 2)))
    w_out = bell_draw(arg_keys[5], (EXPERTS, FF, D), FF ** -0.5, 0.125, ((0, 16), (1, 2)))
    return dict(tokens=tokens, cotangent=cotangent, norm_gain=norm_gain, slot_keys=slot_keys, w_in=w_in, w_out=w_out)


EPSILON = 1e-06

def rounded(values):
    lowered = lax.optimization_barrier(values.astype(jnp.bfloat16))
    return values + lax.stop_gradient(lowered.astype(jnp.float32) - values)

def mixing(tokens_wide, gain, keys_wide):
    average = lax.optimization_barrier(jnp.mean(tokens_wide, axis=-1, keepdims=True))
    centred = tokens_wide - average
    spread = lax.optimization_barrier(jnp.mean(centred * centred, axis=-1, keepdims=True))
    normed = rounded(centred * lax.rsqrt(spread + EPSILON) * gain)
    logits = jnp.einsum('bmd,dn->bmn', normed, keys_wide, precision=lax.Precision.HIGHEST)
    dispatch = rounded(jax.nn.softmax(logits, axis=1))
    combine = jax.nn.softmax(logits, axis=2)
    slot_values = jnp.einsum('bmn,bmd->bnd', dispatch, normed, precision=lax.Precision.HIGHEST)
    return (slot_values, combine)

def expert_forward(slot_rows, first_proj, second_proj):
    pre_act = jnp.dot(slot_rows.astype(jnp.float32), first_proj.astype(jnp.float32), preferred_element_type=jnp.float32)
    hidden = jax.nn.gelu(pre_act).astype(jnp.bfloat16)
    return jnp.dot(hidden.astype(jnp.float32), second_proj.astype(jnp.float32), preferred_element_type=jnp.float32).astype(jnp.bfloat16)

def expert_backward(slot_rows, row_grads, first_proj, second_proj):
    pre_act = jnp.dot(slot_rows.astype(jnp.float32), first_proj.astype(jnp.float32), preferred_element_type=jnp.float32)
    hidden = jax.nn.gelu(pre_act).astype(jnp.bfloat16)
    grad_hidden = lax.dot_general(row_grads.astype(jnp.float32), second_proj.astype(jnp.float32), (((1,), (1,)), ((), ())), preferred_element_type=jnp.float32)
    grad_pre = jax.vjp(jax.nn.gelu, pre_act)[1](grad_hidden)[0].astype(jnp.bfloat16)
    grad_rows = lax.dot_general(grad_pre.astype(jnp.float32), first_proj.astype(jnp.float32), (((1,), (1,)), ((), ())), preferred_element_type=jnp.float32)
    grad_first = lax.dot_general(slot_rows.astype(jnp.float32), grad_pre.astype(jnp.float32), (((0,), (0,)), ((), ())), preferred_element_type=jnp.float32)
    grad_second = lax.dot_general(hidden.astype(jnp.float32), row_grads.astype(jnp.float32), (((0,), (0,)), ((), ())), preferred_element_type=jnp.float32)
    return (grad_rows.astype(jnp.bfloat16), grad_first.astype(jnp.bfloat16), grad_second.astype(jnp.bfloat16))

def to_experts(per_image, images):
    experts = SLOTS // SLOT_PER
    shaped = per_image.reshape(images, experts, SLOT_PER, D)
    return jnp.transpose(shaped, (1, 0, 2, 3)).reshape(experts, images * SLOT_PER, D)

def from_experts(per_expert, images):
    experts = SLOTS // SLOT_PER
    shaped = per_expert.reshape(experts, images, SLOT_PER, D)
    return jnp.transpose(shaped, (1, 0, 2, 3)).reshape(images // IMG_DEV, IMG_DEV, SLOTS, D)

def reference(tokens, cotangent, norm_gain, slot_keys, w_in, w_out):
    images = tokens.shape[0]
    groups = images // IMG_DEV
    image_blocks = tokens.reshape(groups, IMG_DEV, TOK_IMG, D)
    grad_blocks = cotangent.reshape(groups, IMG_DEV, TOK_IMG, D)
    keys_wide = slot_keys.astype(jnp.float32)

    def forward_block(image_block):
        slot_values, combine = mixing(image_block.astype(jnp.float32), norm_gain, keys_wide)
        return (slot_values.astype(jnp.bfloat16), combine.astype(jnp.bfloat16))
    slot_inputs, combine_low = lax.map(forward_block, image_blocks)
    expert_rows = to_experts(slot_inputs, images)
    slot_outputs = lax.map(lambda inputs: expert_forward(inputs[0], inputs[1], inputs[2]), (expert_rows, w_in, w_out))
    slot_outputs = from_experts(slot_outputs, images)

    def combine_block(inputs):
        comb_block, grad_block, out_block = inputs
        grad_slots = jnp.einsum('bmn,bmd->bnd', comb_block.astype(jnp.float32), grad_block.astype(jnp.float32))
        grad_combine = jnp.einsum('bmd,bnd->bmn', grad_block.astype(jnp.float32), out_block.astype(jnp.float32))
        return (grad_slots.astype(jnp.bfloat16), grad_combine)
    grad_slots, grad_combine = lax.map(combine_block, (combine_low, grad_blocks, slot_outputs))
    grad_rows_in = to_experts(grad_slots, images)
    grad_rows, grad_first, grad_second = lax.map(lambda inputs: expert_backward(inputs[0], inputs[1], inputs[2], inputs[3]), (expert_rows, grad_rows_in, w_in, w_out))
    grad_slot_in = from_experts(grad_rows, images)

    def mixing_back(totals, inputs):
        image_block, grad_block, slot_grad, comb_grad = inputs
        unused, pullback = jax.vjp(mixing, image_block.astype(jnp.float32), norm_gain, keys_wide)
        grad_tok, grad_gain, grad_keys = pullback((slot_grad.astype(jnp.float32), comb_grad))
        result = (grad_block.astype(jnp.float32) + grad_tok).astype(jnp.bfloat16)
        return ((totals[0] + grad_gain, totals[1] + grad_keys), result)
    start_totals = (jnp.zeros((D,), jnp.float32), jnp.zeros((D, SLOTS), jnp.float32))
    totals, grad_tokens = lax.scan(mixing_back, start_totals, (image_blocks, grad_blocks, grad_slot_in, grad_combine))
    return (grad_tokens.reshape(images, TOK_IMG, D), totals[0], totals[1], grad_first, grad_second)
```

```python
import functools
import math

import jax
import jax.numpy as jnp
from jax import lax
from jax.experimental import pallas as pl
from jax.experimental.pallas import tpu as pltpu
from jax.sharding import PartitionSpec as P

MESH = pl.DeviceIdType.MESH
EPSILON = 1e-06
F32 = jnp.float32
BF16 = jnp.bfloat16

IMGS = 6
BATCHES = 3
TOK = 256
D = 1280
SLOTS = 32
EXP = 16
HID = 1280
ROWS = 384
HALF = 640
NT = (((1,), (1,)), ((), ()))
TN = (((0,), (0,)), ((), ()))
OWNERS = 10
STAT = 40
CHUNK = 32


def dot(a, b, dims=(((1,), (0,)), ((), ()))):
    return lax.dot_general(a, b, dims, preferred_element_type=F32)


def to_blocks():
    r = lax.broadcasted_iota(jnp.int32, (128, 128), 0)
    c = lax.broadcasted_iota(jnp.int32, (128, 128), 1)
    want = ((r >> 2) & 1) * 64 + ((r >> 1) & 1) * 32 + (r >> 3) * 2 + (r & 1)
    return jnp.where(c == want, 1.0, 0.0).astype(BF16)


def to_blocks_inverse():
    r = lax.broadcasted_iota(jnp.int32, (128, 128), 0)
    c = lax.broadcasted_iota(jnp.int32, (128, 128), 1)
    want = ((c >> 2) & 1) * 64 + ((c >> 1) & 1) * 32 + (c >> 3) * 2 + (c & 1)
    return jnp.where(r == want, 1.0, 0.0).astype(BF16)


def to_kinds():
    r = lax.broadcasted_iota(jnp.int32, (128, 128), 0)
    c = lax.broadcasted_iota(jnp.int32, (128, 128), 1)
    want = ((r >> 2) & 15) * 8 + (r >> 6) * 4 + (r & 3)
    return jnp.where(c == want, 1.0, 0.0).astype(BF16)


def to_kinds_inverse():
    r = lax.broadcasted_iota(jnp.int32, (128, 128), 0)
    c = lax.broadcasted_iota(jnp.int32, (128, 128), 1)
    want = ((c >> 2) & 15) * 8 + (c >> 6) * 4 + (c & 3)
    return jnp.where(r == want, 1.0, 0.0).astype(BF16)


def nth_offset(j):
    half = lax.div(j, 2)
    return jnp.where(lax.rem(j, 2) == 0, half + 1, 15 - half)


def kernel(
    tok_hbm, cot_hbm, gain_ref, keys_ref, win_hbm, wout_hbm,
    out_hbm, fin_ref, g1_ref, g2_ref,
    tok, cot, normed, win, wout, disp, comb, stat, stage, sendbuf, rbuf,
    srows, grows, srows_t, grows_t, hidden, gpre, psend, precv, own, rsend, rback,
    p1, p2, a1p, a1m, a2p, a2m, a3p, a3m, ya, yb, tb, b1p, b1m, b2p, b2m, b3p, b3m, ysum,
    gn, both, acc, gacc, ar_a, ar_x, ar_y,
    tok_sem, cot_sem, w_sem, out_sem, own_sem,
    as_sem, ar_sem, fs_sem, fr_sem, ps_sem, pr_sem, bs_sem, br_sem,
    ras_sem, rar_sem, rbs_sem, rbr_sem, yas_sem, yar_sem, ybs_sem, ybr_sem,
    ra_s, ra_r, rx_s, rx_r, ry_s, ry_r, rc_s, rc_r,
):
    dp = lax.axis_index("dp")
    e = lax.axis_index("expert")
    t = lax.axis_index("tensor")
    x = lax.div(dp, 2)
    ylo = lax.rem(dp, 2)
    y = t * 2 + ylo
    partner = (dp + 1 - 2 * ylo, e, 1 - t)
    ypeer = (dp + 1 - 2 * ylo, e, t)
    xp1 = lax.rem(x + 1, 4)
    xm1 = lax.rem(x + 3, 4)
    xp2 = lax.rem(x + 2, 4)
    xplus = (xp1 * 2 + ylo, e, t)
    xminus = (xm1 * 2 + ylo, e, t)

    def remote(src, dst, s, r, dev):
        return pltpu.make_async_remote_copy(
            src_ref=src, dst_ref=dst, send_sem=s, recv_sem=r, device_id=dev, device_id_type=MESH
        )

    def xdev(k):
        return (lax.rem(x + k, 4) * 2 + ylo, e, t)

    def ydev(k):
        yy = lax.rem(y + k, 4)
        return (x * 2 + lax.rem(yy, 2), e, lax.div(yy, 2))

    def load(i, c):
        pltpu.make_async_copy(tok_hbm.at[i], tok.at[i], tok_sem.at[i]).start()
        pltpu.make_async_copy(cot_hbm.at[i], cot.at[i], cot_sem.at[i]).start()
        return c

    lax.fori_loop(0, IMGS, load, 0)
    pltpu.make_async_copy(win_hbm.at[0], win, w_sem.at[0]).start()
    pltpu.make_async_copy(wout_hbm.at[0], wout, w_sem.at[1]).start()

    barrier = pltpu.get_barrier_semaphore()

    def greet(k, c):
        pl.semaphore_signal(
            barrier, inc=1, device_id=(dp, lax.rem(e + k, EXP), t), device_id_type=MESH
        )
        return c

    lax.fori_loop(1, EXP, greet, 0)
    for k in (1, 2, 3):
        pl.semaphore_signal(barrier, inc=1, device_id=xdev(k), device_id_type=MESH)
        pl.semaphore_signal(barrier, inc=1, device_id=ydev(k), device_id_type=MESH)

    def forward_image(i, row):
        pltpu.make_async_copy(tok_hbm.at[i], tok.at[i], tok_sem.at[i]).wait()

        def norm_rows(r, c):
            rows = pl.ds(pl.multiple_of(r * CHUNK, CHUNK), CHUNK)
            v = tok[i, rows, :].astype(F32)
            mean = jnp.mean(v, axis=-1, keepdims=True)
            centred = v - mean
            inv = lax.rsqrt(jnp.mean(centred * centred, axis=-1, keepdims=True) + EPSILON)
            stat[i, rows, 0:1] = mean
            stat[i, rows, 1:2] = inv
            normed[i, rows, :] = (centred * inv * gain_ref[...]).astype(BF16)
            return c

        lax.fori_loop(0, TOK // CHUNK, norm_rows, 0)
        logits = dot(keys_ref[...], normed[i], NT)
        shifted = jnp.exp(logits - jnp.max(logits, axis=1, keepdims=True))
        dis = shifted / jnp.sum(shifted, axis=1, keepdims=True)
        raised = jnp.exp(logits - jnp.max(logits, axis=0, keepdims=True))
        com = raised / jnp.sum(raised, axis=0, keepdims=True)
        disp[i] = dis
        comb[i] = com
        here = pl.multiple_of(row * SLOTS, SLOTS)
        stage[pl.ds(here, SLOTS), :] = dot(dis.astype(BF16), normed[i]).astype(BF16)
        pltpu.make_async_copy(cot_hbm.at[i], cot.at[i], cot_sem.at[i]).wait()
        stage[pl.ds(here + 64, SLOTS), :] = dot(com.astype(BF16), cot[i]).astype(BF16)

    def a2a(b, j):
        k = nth_offset(j)
        to = lax.rem(e + k, EXP)
        return remote(
            sendbuf.at[pl.ds(pl.multiple_of(b * 128 + to * 8, 8), 8)],
            rbuf.at[pl.ds(pl.multiple_of(b * 128 + e * 8, 8), 8)],
            as_sem.at[b, j], ar_sem.at[b, j], (dp, to, t),
        )

    def own_copy(b):
        return pltpu.make_async_copy(
            sendbuf.at[pl.ds(pl.multiple_of(b * 128 + e * 8, 8), 8)],
            rbuf.at[pl.ds(pl.multiple_of(b * 128 + e * 8, 8), 8)],
            own_sem.at[b],
        )

    for b in range(BATCHES):

        def image(i, c, b=b):
            forward_image(2 * b + i, i)
            return c

        lax.fori_loop(0, 2, image, 0)
        sendbuf[pl.ds(b * 128, 128), :] = dot(to_blocks(), stage[...]).astype(BF16)
        if b == 0:
            pl.semaphore_wait(barrier, 21)
        own_copy(b).start()

        def send(j, c, b=b):
            a2a(b, j).start()
            return c

        lax.fori_loop(0, 15, send, 0)

    def relay(b, src, n):
        at = pl.multiple_of(b * 128 + src * 8, 8)
        return remote(
            rbuf.at[pl.ds(at, 8)],
            rbuf.at[pl.ds(at + ROWS, 8)],
            fs_sem.at[b, n], fr_sem.at[b, n], partner,
        )

    for b in range(BATCHES):
        own_copy(b).wait()
        relay(b, e, 15).start()

        def forward(j, c, b=b):
            a2a(b, j).wait_recv()
            src = lax.rem(e + EXP - nth_offset(j), EXP)
            relay(b, src, j).start()
            return c

        lax.fori_loop(0, 15, forward, 0)

    for i in range(2):
        pltpu.make_async_copy((win_hbm, wout_hbm)[i].at[0], (win, wout)[i], w_sem.at[i]).wait()

    def arrived(b, c):
        def one(n, c):
            relay(b, e, n).wait_recv()
            return c

        return lax.fori_loop(0, 16, one, c)

    lax.fori_loop(0, BATCHES, arrived, 0)

    def split(b, c):
        v = dot(to_kinds(), rbuf[pl.ds(pl.multiple_of(b * 128, 128), 128), :]).astype(BF16)
        at = pl.ds(pl.multiple_of(b * 64, 64), 64)
        srows[at, :] = v[0:64]
        grows[at, :] = v[64:128]
        return c

    lax.fori_loop(0, 6, split, 0)

    root = math.sqrt(2.0 / math.pi)

    def middle(n, c):
        cols = pl.ds(pl.multiple_of(n * 256, 256), 256)
        pre = dot(srows[...], win[:, cols])
        gh = dot(grows[...], wout[cols, :], NT)
        square = pre * pre
        th = jnp.tanh(root * (pre + 0.044715 * (square * pre)))
        cdf = 0.5 * (1.0 + th)
        hidden[:, cols] = (pre * cdf).astype(BF16)
        slope = cdf + 0.5 * pre * (1.0 - th * th) * (root * (1.0 + 3.0 * 0.044715 * square))
        gpre[:, cols] = (gh * slope).astype(BF16)
        return c

    lax.fori_loop(0, 5, middle, 0)

    def theirs(n, c):
        cols = pl.ds(pl.multiple_of(n * 256, 256), 256)
        o = dot(hidden[192:384, :], wout[:, cols]).astype(BF16)
        g = dot(gpre[192:384, :], win[cols, :], NT).astype(BF16)
        for b in range(BATCHES):
            psend[b * 128 : b * 128 + 64, cols] = o[b * 64 : b * 64 + 64]
            psend[b * 128 + 64 : b * 128 + 128, cols] = g[b * 64 : b * 64 + 64]
        return c

    lax.fori_loop(0, 5, theirs, 0)

    def partial(b):
        at = pl.ds(b * 128, 128)
        return remote(psend.at[at], precv.at[at], ps_sem.at[b], pr_sem.at[b], partner)

    for b in range(BATCHES):
        partial(b).start()

    def ours(n, c):
        cols = pl.ds(pl.multiple_of(n * 256, 256), 256)
        o = dot(hidden[0:192, :], wout[:, cols])
        g = dot(gpre[0:192, :], win[cols, :], NT)
        for b in range(BATCHES):
            own[b * 128 : b * 128 + 64, cols] = o[b * 64 : b * 64 + 64]
            own[b * 128 + 64 : b * 128 + 128, cols] = g[b * 64 : b * 64 + 64]
        return c

    lax.fori_loop(0, 5, ours, 0)

    def turn(n, c):
        cols = pl.ds(pl.multiple_of(n * 128, 128), 128)
        srows_t[cols, :] = srows[:, cols].T
        grows_t[cols, :] = grows[:, cols].T
        return c

    lax.fori_loop(0, 10, turn, 0)

    lo = pl.ds(0, HALF)
    hi = pl.ds(HALF, HALF)

    def rows_a(k):
        return pl.ds(pl.multiple_of(k * 320, 320), 320)

    def rows_b(k, which):
        return pl.ds(pl.multiple_of(k * 320 + which * 160, 160), 160)

    def rows_t(k):
        return pl.ds(pl.multiple_of(k * 160, 160), 160)

    def ring(rows, buf, bufs, s, r):
        one_p, one_m, two_p, two_m, three_p, three_m = bufs
        return dict(
            far_p=remote(buf.at[rows(xp2), lo], one_p, s.at[0], r.at[0], xplus),
            far_m=remote(buf.at[rows(xp2), hi], one_m, s.at[1], r.at[1], xminus),
            raw_p=remote(buf.at[rows(xp1), hi], three_p, s.at[2], r.at[2], xplus),
            raw_m=remote(buf.at[rows(xm1), lo], three_m, s.at[3], r.at[3], xminus),
            sum_p=remote(one_p, two_p, s.at[4], r.at[4], xplus),
            sum_m=remote(one_m, two_m, s.at[5], r.at[5], xminus),
        )

    ring_a = ring(rows_a, p1, (a1p, a1m, a2p, a2m, a3p, a3m), ras_sem, rar_sem)
    ring_b = ring(rows_t, tb, (b1p, b1m, b2p, b2m, b3p, b3m), rbs_sem, rbr_sem)

    def send_y(q, k):
        return remote(p2.at[rows_b(k, 1 - ylo)], yb.at[rows_t(k)], ybs_sem.at[q], ybr_sem.at[q], ypeer)

    chunks = (xp2, xp1, xm1, x)
    for q, k in enumerate(chunks):

        def grads(n, c, k=k):
            cols = pl.ds(pl.multiple_of(n * 256, 256), 256)
            p1[rows_a(k), cols] = dot(srows_t[rows_a(k), :], gpre[:, cols]).astype(BF16)
            p2[rows_a(k), cols] = dot(grows_t[rows_a(k), :], hidden[:, cols]).astype(BF16)
            return c

        lax.fori_loop(0, 5, grads, 0)
        send_y(q, k).start()
        if q == 0:
            ring_a["far_p"].start()
            ring_a["far_m"].start()
        elif q == 1:
            ring_a["raw_p"].start()
        elif q == 2:
            ring_a["raw_m"].start()

    def back(b, j):
        k = nth_offset(j)
        to = lax.rem(e + k, EXP)
        return remote(
            rsend.at[pl.ds(pl.multiple_of(b * 128 + to * 8, 8), 8)],
            rback.at[pl.ds(pl.multiple_of(b * 128 + e * 8, 8), 8)],
            bs_sem.at[b, j], br_sem.at[b, j], (dp, to, t),
        )

    def own_back(b):
        return pltpu.make_async_copy(
            rsend.at[pl.ds(pl.multiple_of(b * 128 + e * 8, 8), 8)],
            rback.at[pl.ds(pl.multiple_of(b * 128 + e * 8, 8), 8)],
            own_sem.at[b],
        )

    def give_back(b):
        at = pl.ds(b * 128, 128)
        partial(b).wait_recv()
        whole = (own[at, :] + precv[at, :].astype(F32)).astype(BF16)
        rsend[at, :] = dot(to_kinds_inverse(), whole).astype(BF16)
        own_back(b).start()

        def send(j, c):
            back(b, j).start()
            return c

        lax.fori_loop(0, 15, send, 0)

    def add_rows(dst, parts, count):
        def step(r, c):
            rows = pl.ds(pl.multiple_of(r * 32, 32), 32)
            total = parts[0](rows).astype(F32)
            for p in parts[1:]:
                total = total + p(rows).astype(F32)
            dst(rows, total.astype(BF16))
            return c

        lax.fori_loop(0, count // 32, step, 0)

    def pass_on(rg, buf, base, one_p, one_m, count):
        rg["far_p"].wait_recv()

        def put_p(rows, v):
            one_p[rows, :] = v

        add_rows(
            put_p,
            (lambda r: one_p[r, :], lambda r: buf[pl.ds(base(xp1) + r.start, 32), lo]),
            count,
        )
        rg["sum_p"].start()
        rg["far_m"].wait_recv()

        def put_m(rows, v):
            one_m[rows, :] = v

        add_rows(
            put_m,
            (lambda r: one_m[r, :], lambda r: buf[pl.ds(base(xm1) + r.start, 32), hi]),
            count,
        )
        rg["sum_m"].start()

    def base_a(k):
        return pl.multiple_of(k * 320, 32)

    def base_t(k):
        return pl.multiple_of(k * 160, 32)

    def take_y(q, k):
        send_y(q, k).wait_recv()

        def put(rows, v):
            tb[pl.ds(base_t(k) + rows.start, 32), :] = v

        add_rows(
            put,
            (
                lambda r: yb[pl.ds(base_t(k) + r.start, 32), :],
                lambda r: p2[pl.ds(pl.multiple_of(k * 320 + ylo * 160, 32) + r.start, 32), :],
            ),
            160,
        )

    give_back(0)
    pass_on(ring_a, p1, base_a, a1p, a1m, 320)
    take_y(0, xp2)
    ring_b["far_p"].start()
    ring_b["far_m"].start()
    give_back(1)
    take_y(1, xp1)
    ring_b["raw_p"].start()
    give_back(2)

    acc[...] = jnp.zeros_like(acc)
    gacc[...] = jnp.zeros_like(gacc)

    def backward_image(i, row):
        here = pl.multiple_of(row * SLOTS, SLOTS)
        outs = stage[pl.ds(here, SLOTS), :]
        gin = stage[pl.ds(here + 64, SLOTS), :]
        gc = dot(outs, cot[i], NT)
        gd = dot(gin, normed[i], NT)
        dis = disp[i]
        com = comb[i]
        gl = dis * (gd - jnp.sum(dis * gd, axis=1, keepdims=True))
        gl = gl + com * (gc - jnp.sum(com * gc, axis=0, keepdims=True))
        high = gl.astype(BF16)
        low = (gl - high.astype(F32)).astype(BF16)
        terms = jnp.concatenate([high, low], axis=0)
        kt = dot(terms, normed[i])
        acc[0:SLOTS, :] += kt[0:SLOTS] + kt[SLOTS : 2 * SLOTS]
        both[0:SLOTS, :] = gin
        left = jnp.concatenate([dis.astype(BF16), high, low], axis=0)
        gn[...] = dot(left, both[...], TN)

        def rows_of(r, c):
            rows = pl.ds(pl.multiple_of(r * CHUNK, CHUNK), CHUNK)
            mean = stat[i, rows, 0:1]
            inv = stat[i, rows, 1:2]
            g = gn[rows, :]
            scaled = (tok[i, rows, :].astype(F32) - mean) * inv
            prod = g * scaled
            gacc[...] += jnp.sum(prod.reshape(CHUNK // 8, 8, D), axis=0)
            gain = gain_ref[...]
            gs = g * gain
            m1 = jnp.mean(gs, axis=-1, keepdims=True)
            m2 = jnp.mean(prod * gain, axis=-1, keepdims=True)
            res = cot[i, rows, :].astype(F32) + inv * (gs - m1 - scaled * m2)
            normed[i, rows, :] = res.astype(BF16)
            return c

        lax.fori_loop(0, TOK // CHUNK, rows_of, 0)
        pltpu.make_async_copy(normed.at[i], out_hbm.at[i], out_sem.at[i]).start()

    both[SLOTS : 2 * SLOTS, :] = keys_ref[...]
    both[2 * SLOTS : 3 * SLOTS, :] = keys_ref[...]

    def backward_batch(b):
        own_back(b).wait()

        def one(j, c):
            back(b, j).wait_recv()
            return c

        lax.fori_loop(0, 15, one, 0)
        stage[...] = dot(to_blocks_inverse(), rback[pl.ds(b * 128, 128), :]).astype(BF16)

        def image(i, c):
            backward_image(2 * b + i, i)
            return c

        lax.fori_loop(0, 2, image, 0)

    backward_batch(0)
    take_y(2, xm1)
    ring_b["raw_m"].start()
    pass_on(ring_b, tb, base_t, b1p, b1m, 160)
    backward_batch(1)
    take_y(3, x)
    backward_batch(2)

    acc[SLOTS : SLOTS + 8, :] = jnp.sum(gacc[...], axis=0, keepdims=True) * jnp.where(
        lax.broadcasted_iota(jnp.int32, (8, 1), 0) == 0, 1.0, 0.0
    )

    def cols_of(k):
        return pl.ds(pl.multiple_of(k * 128, 128), 128)

    def to_owner(k):
        to = lax.rem(e + k, EXP)
        return to, remote(
            acc.at[:, cols_of(lax.rem(to, OWNERS))], ar_a.at[k], ra_s.at[k], ra_r.at[k], (dp, to, t)
        )

    def send_owner(k, c):
        to, copy = to_owner(k)

        @pl.when(to < OWNERS)
        def _():
            copy.start()

        return c

    lax.fori_loop(1, EXP, send_owner, 0)

    def finish(rg, buf, base, two_p, two_m, three_p, three_m, count, dst):
        rg["sum_p"].wait_recv()
        rg["raw_m"].wait_recv()

        def put_lo(rows, v):
            dst[rows, lo] = v

        def put_hi(rows, v):
            dst[rows, hi] = v

        add_rows(
            put_lo,
            (
                lambda r: buf[pl.ds(base(x) + r.start, 32), lo],
                lambda r: two_p[r, :],
                lambda r: three_m[r, :],
            ),
            count,
        )
        rg["sum_m"].wait_recv()
        rg["raw_p"].wait_recv()
        add_rows(
            put_hi,
            (
                lambda r: buf[pl.ds(base(x) + r.start, 32), hi],
                lambda r: two_m[r, :],
                lambda r: three_p[r, :],
            ),
            count,
        )

    finish(ring_a, p1, base_a, a2p, a2m, a3p, a3m, 320, ysum)
    mine = pl.multiple_of(ylo * 160, 160)
    other = pl.multiple_of((1 - ylo) * 160, 160)
    last = remote(ysum.at[pl.ds(other, 160)], ya, yas_sem, yar_sem, ypeer)
    last.start()

    @pl.when(e < OWNERS)
    def _():
        ar_x[x] = acc[:, cols_of(lax.rem(e, OWNERS))]

        def gather(k, c):
            to_owner(k)[1].wait_recv()
            ar_x[x] += ar_a[k]
            return c

        lax.fori_loop(1, EXP, gather, 0)
        for k in (1, 2, 3):
            remote(ar_x.at[x], ar_x.at[x], rx_s.at[k], rx_r.at[k], xdev(k)).start()
        for k in (1, 2, 3):
            src = lax.rem(x + 4 - k, 4)
            remote(ar_x.at[src], ar_x.at[src], rx_s.at[k], rx_r.at[k], xdev(k)).wait_recv()
        ar_y[y] = ar_x[0] + ar_x[1] + ar_x[2] + ar_x[3]
        for k in (1, 2, 3):
            remote(ar_y.at[y], ar_y.at[y], ry_s.at[k], ry_r.at[k], ydev(k)).start()
        for k in (1, 2, 3):
            src = lax.rem(y + 4 - k, 4)
            remote(ar_y.at[src], ar_y.at[src], ry_s.at[k], ry_r.at[k], ydev(k)).wait_recv()
        cols = cols_of(lax.rem(e, OWNERS))
        fin_ref[:, cols] = ar_y[0] + ar_y[1] + ar_y[2] + ar_y[3]

        def hand(k, c):
            to = lax.rem(e + k, EXP)
            remote(fin_ref.at[:, cols], fin_ref.at[:, cols], rc_s.at[k], rc_r.at[k], (dp, to, t)).start()
            return c

        lax.fori_loop(1, EXP, hand, 0)

    finish(ring_b, tb, base_t, b2p, b2m, b3p, b3m, 160, g2_ref)
    last.wait_recv()

    def put_g1(rows, v):
        g1_ref[rows, :] = v

    add_rows(
        put_g1,
        (lambda r: ysum[pl.ds(mine + r.start, 32), :], lambda r: ya[r, :]),
        160,
    )

    def taken(k, c):
        src = lax.rem(e + EXP - k, EXP)

        @pl.when(src < OWNERS)
        def _():
            cols = cols_of(lax.rem(src, OWNERS))
            remote(fin_ref.at[:, cols], fin_ref.at[:, cols], rc_s.at[k], rc_r.at[k], (dp, src, t)).wait_recv()

        return c

    lax.fori_loop(1, EXP, taken, 0)

    def drain(b, c):
        def one(j, c):
            a2a(b, j).wait_send()
            back(b, j).wait_send()
            relay(b, e, j).wait_send()
            return c

        lax.fori_loop(0, 15, one, c)
        relay(b, e, 15).wait_send()
        return c

    lax.fori_loop(0, BATCHES, drain, 0)
    for b in range(BATCHES):
        partial(b).wait_send()
    for q, k in enumerate(chunks):
        send_y(q, k).wait_send()
    for rg in (ring_a, ring_b):
        for copy in rg.values():
            copy.wait_send()
    last.wait_send()

    def drain_owner(k, c):
        to, copy = to_owner(k)

        @pl.when(to < OWNERS)
        def _():
            copy.wait_send()

        return c

    lax.fori_loop(1, EXP, drain_owner, 0)

    @pl.when(e < OWNERS)
    def _():
        for k in (1, 2, 3):
            remote(ar_x.at[x], ar_x.at[x], rx_s.at[k], rx_r.at[k], xdev(k)).wait_send()
            remote(ar_y.at[y], ar_y.at[y], ry_s.at[k], ry_r.at[k], ydev(k)).wait_send()
        cols = cols_of(lax.rem(e, OWNERS))

        def sent(k, c):
            to = lax.rem(e + k, EXP)
            remote(fin_ref.at[:, cols], fin_ref.at[:, cols], rc_s.at[k], rc_r.at[k], (dp, to, t)).wait_send()
            return c

        lax.fori_loop(1, EXP, sent, 0)

    def drain_out(i, c):
        pltpu.make_async_copy(normed.at[i], out_hbm.at[i], out_sem.at[i]).wait()
        return c

    lax.fori_loop(0, IMGS, drain_out, 0)


def local(tokens, cotangent, norm_gain, slot_keys, w_in, w_out):
    V = pltpu.VMEM
    S = pltpu.SemaphoreType.DMA
    any_ = pl.BlockSpec(memory_space=pl.ANY)
    vm = pl.BlockSpec(memory_space=pltpu.VMEM)
    scratch = [
        V((IMGS, TOK, D), BF16), V((IMGS, TOK, D), BF16), V((IMGS, TOK, D), BF16),
        V((D, HID), BF16), V((HID, D), BF16),
        V((IMGS, SLOTS, TOK), F32), V((IMGS, SLOTS, TOK), F32), V((IMGS, TOK, 128), F32),
        V((128, D), BF16), V((ROWS, D), BF16), V((2 * ROWS, D), BF16),
        V((ROWS, D), BF16), V((ROWS, D), BF16), V((D, ROWS), BF16), V((D, ROWS), BF16),
        V((ROWS, HID), BF16), V((ROWS, HID), BF16),
        V((ROWS, D), BF16), V((ROWS, D), BF16), V((ROWS, D), F32), V((ROWS, D), BF16), V((ROWS, D), BF16),
        V((D, HID), BF16), V((D, HID), BF16),
    ]
    scratch += [V((320, HALF), BF16)] * 6
    scratch += [V((160, D), BF16), V((HALF, D), BF16), V((HALF, D), BF16)]
    scratch += [V((160, HALF), BF16)] * 6
    scratch += [
        V((320, D), BF16),
        V((TOK, D), F32), V((96, D), BF16), V((STAT, D), F32), V((8, D), F32),
        V((EXP, STAT, 128), F32), V((4, STAT, 128), F32), V((4, STAT, 128), F32),
    ]
    scratch += [
        S((IMGS,)), S((IMGS,)), S((2,)), S((IMGS,)), S((BATCHES,)),
        S((BATCHES, 15)), S((BATCHES, 15)), S((BATCHES, 16)), S((BATCHES, 16)),
        S((BATCHES,)), S((BATCHES,)), S((BATCHES, 15)), S((BATCHES, 15)),
        S((6,)), S((6,)), S((6,)), S((6,)), S(()), S(()), S((4,)), S((4,)),
        S((EXP,)), S((EXP,)), S((4,)), S((4,)), S((4,)), S((4,)), S((EXP,)), S((EXP,)),
    ]
    out, fin, g1, g2 = pl.pallas_call(
        kernel,
        name="moe_block",
        out_shape=(
            jax.ShapeDtypeStruct((IMGS, TOK, D), BF16),
            jax.ShapeDtypeStruct((STAT, D), F32),
            jax.ShapeDtypeStruct((160, HID), BF16),
            jax.ShapeDtypeStruct((160, HID), BF16),
        ),
        in_specs=[any_, any_, vm, vm, any_, any_],
        out_specs=(any_, vm, vm, vm),
        scratch_shapes=scratch,
        compiler_params=pltpu.CompilerParams(
            collective_id=0, has_side_effects=True, vmem_limit_bytes=67043328
        ),
    )(tokens, cotangent, norm_gain[None], slot_keys.T, w_in, w_out)
    return out, fin[SLOTS], fin[:SLOTS].T, g1[None], g2.T[None]


def solution(mesh):
    images = P(("dp", "expert", "tensor"), None, None)
    return jax.shard_map(
        local,
        mesh=mesh,
        in_specs=(images, images, P(), P(), P("expert", None, "tensor"), P("expert", "tensor", None)),
        out_specs=(images, P(), P(), P("expert", "dp", "tensor"), P("expert", "tensor", "dp")),
        check_vma=False,
    )
```
